32 devices in a mesh: mem: 8 (over z, x), grid: 4 (over y, core).
Axes of the slice: x: 2, y: 2, z: 4, core: 2. Of those that a mesh axis runs over, the one named last changes fastest.
Arguments:
- alpha: bfloat16 [16, 8, 768, 1536], P('mem', None, 'grid'), may hold values from -6 to 6
- perturbation: bfloat16 [16, 8, 768, 1536], P('mem', None, 'grid'), may hold values from -6 to 6
- legendre: bfloat16 [192, 128, 768], P('grid'), may hold values from -0.21875 to 0.21875
- response: float32 [192, 128], P('grid'), may hold values from 0.2 to 2
Outputs:
- increment: float32 [8, 768, 1536], P('mem', 'grid')
The draws below stay inside these ranges and needn't reach their ends.
All inputs are finite; a program needn't handle non-finite values.
Results may differ from the reference program's by a relative error of at most 0.0063.
Values may be sent and summed in bfloat16 or wider, within the bound.
A program may use at most 128 MiB of HBM per device.

```python
import math
import jax
import jax.numpy as jnp
from jax import lax

NLON = 1536
NLAT = 768
KEEP = 192
NN = 128
MEMBERS = 16
LEV = 8


def block_scale(stream_key, extent, split, least, top_value):
    def one(axis_at, blocks):
        heights = jax.random.uniform(jax.random.fold_in(jax.random.fold_in(stream_key, 6), axis_at), (blocks,), jnp.float32, least / len(split), top_value / len(split))
        return jnp.repeat(jnp.exp(heights), extent[axis_at] // blocks).reshape((-1,) + (1,) * (len(extent) - axis_at - 1))

    level = one(*split[0])
    for cut in split[1:]:
        level = level * one(*cut)
    return level


def gaussian(stream_key, extent, deviation, most, pieces=(), kind=jnp.bfloat16):
    result = deviation * jax.random.normal(stream_key, extent, jnp.float32)
    if pieces:
        result = result * block_scale(stream_key, extent, pieces, -0.22, 0.18)
    return jnp.clip(result, -most, most).astype(kind)


def setup_inputs(seed: int = 0) -> dict:
    streams_of = jax.random.split(jax.random.key(seed), 5)
    return {
        "alpha": gaussian(streams_of[0], (MEMBERS, LEV, NLAT, NLON), 1.0, 6.0, ((0, 8), (2, 4))),
        "perturbation": gaussian(streams_of[1], (MEMBERS, LEV, NLAT, NLON), 1.0, 6.0, ((0, 8), (2, 4))),
        "legendre": gaussian(streams_of[2], (KEEP, NN, NLAT), NLAT ** -0.5, 0.21875, ((0, 4),)),
        "response": jnp.clip(jnp.exp(math.log(2.0) - 2.3025851 * jax.random.uniform(streams_of[3], (KEEP, NN), jnp.float32) ** block_scale(streams_of[3], (KEEP, NN), ((0, 4),), -0.2, 0.2)), 0.2, 2.0),
    }


def build_tables(lon_count, keep):
    col = jnp.arange(2 * keep, dtype=jnp.int32)
    part = col // keep
    wave = col % keep
    lon = jnp.arange(lon_count, dtype=jnp.int32)
    phase = lon[:, None] * wave[None, :] % lon_count
    angle = phase.astype(jnp.float32) * jnp.float32(2.0 * math.pi / lon_count)
    basis = jnp.where(part[None, :] == 0, jnp.cos(angle), jnp.sin(angle))
    weight = jnp.where(wave == 0, jnp.float32(1.0), jnp.float32(2.0)) / jnp.float32(lon_count)
    forward = basis.astype(jnp.bfloat16)
    inverse = jnp.transpose(basis * weight[None, :]).astype(jnp.bfloat16)
    return (forward, inverse)

def reference(alpha, perturbation, legendre, response):
    members = alpha.shape[0]
    forward, inverse = build_tables(NLON, KEEP)
    legendre_wide = legendre.astype(jnp.float32)

    def one_member(total, pair):
        field, pert = pair
        spec = jnp.dot(field.reshape(LEV * NLAT, NLON), forward, preferred_element_type=jnp.float32)
        spec = spec.astype(jnp.bfloat16).reshape(LEV, NLAT, 2, KEEP)
        coef = jnp.einsum('mnt,ltqm->lqmn', legendre_wide, spec.astype(jnp.float32))
        coef = (coef * response[None, None, :, :]).astype(jnp.bfloat16)
        synth = jnp.einsum('mnt,lqmn->ltqm', legendre_wide, coef.astype(jnp.float32)).astype(jnp.bfloat16)
        values = jnp.dot(synth.reshape(LEV * NLAT, 2 * KEEP), inverse, preferred_element_type=jnp.float32)
        values = values.reshape(LEV, NLAT, NLON)
        return (total + values * pert.astype(jnp.float32), None)
    start = jnp.zeros((LEV, NLAT, NLON), jnp.float32)
    total, unused = lax.scan(one_member, start, (alpha, perturbation))
    return total / jnp.sqrt(jnp.float32(members - 1))
```

```python
import functools
import math

import jax
import jax.numpy as jnp
import numpy as np
from jax import lax
from jax.experimental import pallas as pl
from jax.experimental.pallas import tpu as pltpu
from jax.sharding import PartitionSpec as P


def build_table(lon_count, keep_dev, grid_count):
    col = np.arange(2 * keep_dev * grid_count)
    block = col // (2 * keep_dev)
    part = col // keep_dev % 2
    wave = block * keep_dev + col % keep_dev
    phase = wave[:, None] * np.arange(lon_count)[None, :] % lon_count
    angle = phase.astype(np.float32) * np.float32(2.0 * math.pi / lon_count)
    basis = np.where(part[:, None] == 0, np.cos(angle), np.sin(angle))
    return jnp.asarray(basis.astype(jnp.bfloat16))


def legendre_filter(split, legendre, response):
    coef = jnp.einsum("mnt,qmkit->qmkin", legendre, split, preferred_element_type=jnp.float32)
    coef = (coef * response[None, :, None, None, :]).astype(jnp.bfloat16)
    synth = jnp.einsum("mnt,qmkin->qmkit", legendre, coef, preferred_element_type=jnp.float32)
    return synth.astype(jnp.bfloat16)


def reduce_levels(partial, levels):
    mem_count = lax.axis_size("mem")
    me = lax.axis_index("mem")
    owned = levels // mem_count
    if mem_count % 2:
        every = jnp.concatenate([partial(i * owned, owned) for i in range(mem_count)])
        return lax.psum_scatter(every, "mem", scatter_dimension=0, tiled=True)
    ring = mem_count // 2
    side, place = me % 2, me // 2
    swap = [(j, j ^ 1) for j in range(mem_count)]
    onward = [(j, (j + 2) % mem_count) for j in range(mem_count)]
    total = None
    for step in range(ring):
        goal = (place + 2 * ring - 1 - step) % ring
        give = partial((2 * goal + 1 - side) * owned, owned).astype(jnp.bfloat16)
        got = lax.ppermute(give, "mem", swap)
        here = partial((2 * goal + side) * owned, owned)
        here = here + got.astype(jnp.float32)
        if total is not None:
            here = here + total.astype(jnp.float32)
        if step < ring - 1:
            total = lax.ppermute(here.astype(jnp.bfloat16), "mem", onward)
    return here


def filter_kernel(lat_dev, x_ref, legendre_ref, response_ref, out_ref, rows_ref, back_ref):
    grid_count, parts, waves, points = x_ref.shape
    tiles = points // 128
    per_pair = 2 * lat_dev // 128
    pairs = tiles // per_pair
    half = per_pair // 2
    for src in range(grid_count):
        for part in range(parts):
            for tile in range(tiles):
                spot = (tile % per_pair) * pairs + tile // per_pair
                rows_ref[src, part, spot * waves : (spot + 1) * waves, :] = x_ref[
                    src, part, :, tile * 128 : (tile + 1) * 128
                ].astype(jnp.float32)

    def one_wave(wave, carry):
        lines = []
        for part in range(parts):
            even, odd = [], []
            for src in range(grid_count):
                block = rows_ref[src, part, pl.ds(wave, tiles, stride=waves), :]
                piece = [block[i * pairs : (i + 1) * pairs] for i in range(per_pair)]
                even += piece[:half] + [piece[half][:, :64]]
                odd += [piece[half][:, 64:]] + piece[half + 1 :]
            lines += [jnp.concatenate(even, axis=1), jnp.concatenate(odd, axis=1)]
        field = jnp.concatenate(lines, axis=0).astype(jnp.bfloat16)
        basis = legendre_ref[wave]
        coef = lax.dot_general(
            field, basis, (((1,), (1,)), ((), ())), preferred_element_type=jnp.float32
        )
        coef = (coef * response_ref[pl.ds(wave, 1), :]).astype(jnp.bfloat16)
        synth = jnp.dot(coef, basis, preferred_element_type=jnp.float32)
        for part in range(parts):
            even = synth[2 * part * pairs : (2 * part + 1) * pairs]
            odd = synth[(2 * part + 1) * pairs : (2 * part + 2) * pairs]
            for src in range(grid_count):
                base = src * lat_dev
                both = jnp.concatenate(
                    [even[:, base : base + lat_dev], odd[:, base : base + lat_dev]], axis=1
                )
                block = jnp.concatenate(
                    [both[:, i * 128 : (i + 1) * 128] for i in range(per_pair)], axis=0
                )
                back_ref[src, part, pl.ds(wave, tiles, stride=waves), :] = block
        return carry

    lax.fori_loop(0, waves, one_wave, 0)
    for src in range(grid_count):
        for part in range(parts):
            for tile in range(tiles):
                spot = (tile % per_pair) * pairs + tile // per_pair
                out_ref[src, part, :, tile * 128 : (tile + 1) * 128] = back_ref[
                    src, part, spot * waves : (spot + 1) * waves, :
                ].astype(jnp.bfloat16)


def filter_packed(spectra, legendre, response, lat_dev, start, count):
    grid_count, parts, _, points = spectra.shape
    degrees, lat_count = legendre.shape[1:]
    waves = 16
    first = start // waves
    block = pl.BlockSpec((grid_count, parts, waves, points), lambda i: (0, 0, i, 0))
    return pl.pallas_call(
        functools.partial(filter_kernel, lat_dev),
        out_shape=jax.ShapeDtypeStruct(spectra.shape, jnp.bfloat16),
        grid=(count // waves,),
        in_specs=[
            block,
            pl.BlockSpec((waves, degrees, lat_count), lambda i: (i + first, 0, 0)),
            pl.BlockSpec((waves, degrees), lambda i: (i + first, 0)),
        ],
        out_specs=block,
        scratch_shapes=[
            pltpu.VMEM((grid_count, parts, points // 128 * waves, 128), jnp.float32),
            pltpu.VMEM((grid_count, parts, points // 128 * waves, 128), jnp.float32),
        ],
        compiler_params=pltpu.CompilerParams(vmem_limit_bytes=40 * 2**20),
        cost_estimate=pl.CostEstimate(
            flops=8 * count * degrees * lat_count * points // lat_dev,
            bytes_accessed=2 * count * degrees * lat_count,
            transcendentals=0,
        ),
    )(spectra, legendre, response)


def synth_kernel(where_ref, field_ref, table_ref, weight_ref, give_ref, keep_ref, total_ref):
    member = pl.program_id(1)
    side = where_ref[1]
    pair, lat_dev, wide = total_ref.shape
    values = lax.dot_general(
        field_ref[...], table_ref[...], (((0,), (0,)), ((), ())), preferred_element_type=jnp.float32
    ).reshape(pair, lat_dev, wide)
    term = values * weight_ref[0].astype(jnp.float32)

    @pl.when(member == 0)
    def _():
        total_ref[...] = term

    @pl.when(member > 0)
    def _():
        total_ref[...] += term

    @pl.when(member == pl.num_programs(1) - 1)
    def _():
        give_ref[0] = total_ref[1 - side].astype(jnp.bfloat16)
        keep_ref[0] = total_ref[side]


def synth_pair(filtered, table, perturbation, goal, side):
    mem_dev, levels, lat_dev, lon_count = perturbation.shape
    cols = table.shape[0]
    pairs = levels // 2
    wide = math.gcd(lon_count, 512)
    level = pl.BlockSpec((1, lat_dev, wide), lambda i, k, w: (0, 0, i))
    return pl.pallas_call(
        synth_kernel,
        out_shape=(
            jax.ShapeDtypeStruct((1, lat_dev, lon_count), jnp.bfloat16),
            jax.ShapeDtypeStruct((1, lat_dev, lon_count), jnp.float32),
        ),
        grid_spec=pltpu.PrefetchScalarGridSpec(
            num_scalar_prefetch=1,
            grid=(lon_count // wide, mem_dev),
            in_specs=[
                pl.BlockSpec((cols, 2 * lat_dev), lambda i, k, w: (0, k * pairs + w[0])),
                pl.BlockSpec((cols, wide), lambda i, k, w: (0, i)),
                pl.BlockSpec((1, 2, lat_dev, wide), lambda i, k, w: (k, w[0], 0, i)),
            ],
            out_specs=(level, level),
            scratch_shapes=[pltpu.VMEM((2, lat_dev, wide), jnp.float32)],
        ),
        compiler_params=pltpu.CompilerParams(vmem_limit_bytes=24 * 2**20),
        cost_estimate=pl.CostEstimate(
            flops=4 * mem_dev * lat_dev * cols * lon_count,
            bytes_accessed=4 * mem_dev * lat_dev * lon_count,
            transcendentals=0,
        ),
    )(jnp.stack([goal, side]).astype(jnp.int32), filtered, table, perturbation)


def reduce_pairs(both):
    mem_count = lax.axis_size("mem")
    me = lax.axis_index("mem")
    ring = mem_count // 2
    side, place = me % 2, me // 2
    swap = [(j, j ^ 1) for j in range(mem_count)]
    onward = [(j, (j + 2) % mem_count) for j in range(mem_count)]
    total = None
    for step in range(ring):
        goal = (place + 2 * ring - 1 - step) % ring
        give, here = both(goal, side)
        here = here + lax.ppermute(give, "mem", swap).astype(jnp.float32)
        if total is not None:
            here = here + total.astype(jnp.float32)
        if step < ring - 1:
            total = lax.ppermute(here.astype(jnp.bfloat16), "mem", onward)
    return here


def packed(alpha, perturbation, legendre, response, table):
    mem_dev, levels, lat_dev, lon_count = alpha.shape
    keep_dev = legendre.shape[0]
    grid_count = lax.axis_size("grid")
    points = mem_dev * levels * lat_dev
    spectra = lax.dot_general(
        table, alpha.reshape(points, lon_count), (((1,), (1,)), ((), ())), preferred_element_type=jnp.float32
    ).astype(jnp.bfloat16)
    spectra = spectra.reshape(grid_count, 2, keep_dev, points)
    chunks = CHUNKS
    step = keep_dev // chunks
    pieces = []
    for i in range(chunks):
        piece = spectra[:, :, i * step : (i + 1) * step].reshape(grid_count, 2 * step, points)
        piece = lax.all_to_all(piece, "grid", split_axis=0, concat_axis=0, tiled=True)
        piece = piece.reshape(grid_count, 2, step, points)
        piece = filter_packed(piece, legendre, response, lat_dev, i * step, step)
        piece = piece.reshape(grid_count, 2 * step, points)
        piece = lax.all_to_all(piece, "grid", split_axis=0, concat_axis=0, tiled=True)
        pieces.append(piece.reshape(grid_count, 2, step, points))
    filtered = jnp.concatenate(pieces, axis=2).reshape(grid_count * 2 * keep_dev, points)
    return reduce_pairs(lambda goal, side: synth_pair(filtered, table, perturbation, goal, side))


CHUNKS = 1


def body(alpha, perturbation, legendre, response):
    mem_dev, levels, lat_dev, lon_count = alpha.shape
    keep_dev = legendre.shape[0]
    grid_count = lax.axis_size("grid")
    members = mem_dev * lax.axis_size("mem")
    cols = 2 * keep_dev
    table = build_table(lon_count, keep_dev, grid_count)
    wave = lax.axis_index("grid") * keep_dev + jnp.arange(keep_dev)
    response = response * jnp.where(wave == 0, 1.0, 2.0).astype(jnp.float32)[:, None]

    scale = jnp.float32(1.0 / (lon_count * math.sqrt(members - 1)))
    if keep_dev % 16 == 0 and lat_dev % 128 == 64 and levels == lax.axis_size("mem") and levels % 2 == 0:
        return packed(alpha, perturbation, legendre, response, table) * scale

    points = mem_dev * levels * lat_dev
    lane = math.gcd(points, 128)
    spectra = jnp.einsum("cx,klyx->ckly", table, alpha, preferred_element_type=jnp.float32)
    spectra = spectra.astype(jnp.bfloat16).reshape(grid_count, cols, points // lane, lane)
    spectra = lax.all_to_all(spectra, "grid", split_axis=0, concat_axis=0, tiled=True)
    split = spectra.reshape(grid_count, 2, keep_dev, mem_dev, levels, lat_dev)
    split = jnp.transpose(split, (1, 2, 3, 4, 0, 5)).reshape(2, keep_dev, mem_dev, levels, -1)
    filtered = legendre_filter(split, legendre, response)
    filtered = filtered.reshape(2, keep_dev, mem_dev, levels, grid_count, lat_dev)
    filtered = jnp.transpose(filtered, (4, 0, 1, 2, 3, 5)).reshape(grid_count, cols, points // lane, lane)
    filtered = lax.all_to_all(filtered, "grid", split_axis=0, concat_axis=0, tiled=True)
    filtered = filtered.reshape(grid_count * cols, mem_dev, levels, lat_dev)
    filtered = jnp.transpose(filtered, (1, 2, 3, 0))

    def partial(level, count):
        field = lax.dynamic_slice_in_dim(filtered, level, count, 1)
        weight = lax.dynamic_slice_in_dim(perturbation, level, count, 1)
        values = jnp.einsum("klyc,cx->klyx", field, table, preferred_element_type=jnp.float32)
        return jnp.sum(values * weight, axis=0)

    total = reduce_levels(partial, levels)
    return total * scale


def solution(mesh):
    placed = (
        P("mem", None, "grid", None),
        P("mem", None, "grid", None),
        P("grid", None, None),
        P("grid", None),
    )
    return jax.shard_map(
        body, mesh=mesh, in_specs=placed, out_specs=P("mem", "grid", None), check_vma=False
    )
```

```python
import functools
import math

import jax
import jax.numpy as jnp
import numpy as np
from jax import lax
from jax.experimental import pallas as pl
from jax.experimental.pallas import tpu as pltpu
from jax.sharding import PartitionSpec as P


def build_table(lon_count, keep_dev, grid_count):
    col = np.arange(2 * keep_dev * grid_count)
    block = col // (2 * keep_dev)
    part = col // keep_dev % 2
    wave = block * keep_dev + col % keep_dev
    phase = wave[:, None] * np.arange(lon_count)[None, :] % lon_count
    angle = phase.astype(np.float32) * np.float32(2.0 * math.pi / lon_count)
    basis = np.where(part[:, None] == 0, np.cos(angle), np.sin(angle))
    return jnp.asarray(basis.astype(jnp.bfloat16))


def legendre_filter(split, legendre, response):
    coef = jnp.einsum("mnt,qmkit->qmkin", legendre, split, preferred_element_type=jnp.float32)
    coef = (coef * response[None, :, None, None, :]).astype(jnp.bfloat16)
    synth = jnp.einsum("mnt,qmkin->qmkit", legendre, coef, preferred_element_type=jnp.float32)
    return synth.astype(jnp.bfloat16)


def reduce_levels(partial, levels):
    mem_count = lax.axis_size("mem")
    me = lax.axis_index("mem")
    owned = levels // mem_count
    if mem_count % 2:
        every = jnp.concatenate([partial(i * owned, owned) for i in range(mem_count)])
        return lax.psum_scatter(every, "mem", scatter_dimension=0, tiled=True)
    ring = mem_count // 2
    side, place = me % 2, me // 2
    swap = [(j, j ^ 1) for j in range(mem_count)]
    onward = [(j, (j + 2) % mem_count) for j in range(mem_count)]
    total = None
    for step in range(ring):
        goal = (place + 2 * ring - 1 - step) % ring
        give = partial((2 * goal + 1 - side) * owned, owned).astype(jnp.bfloat16)
        got = lax.ppermute(give, "mem", swap)
        here = partial((2 * goal + side) * owned, owned)
        here = here + got.astype(jnp.float32)
        if total is not None:
            here = here + total.astype(jnp.float32)
        if step < ring - 1:
            total = lax.ppermute(here.astype(jnp.bfloat16), "mem", onward)
    return here


def filter_kernel(lat_dev, x_ref, legendre_ref, response_ref, out_ref, rows_ref, back_ref):
    grid_count, parts, waves, points = x_ref.shape
    tiles = points // 128
    per_pair = 2 * lat_dev // 128
    pairs = tiles // per_pair
    half = per_pair // 2
    for src in range(grid_count):
        for part in range(parts):
            for tile in range(tiles):
                spot = (tile % per_pair) * pairs + tile // per_pair
                rows_ref[src, part, spot * waves : (spot + 1) * waves, :] = x_ref[
                    src, part, :, tile * 128 : (tile + 1) * 128
                ].astype(jnp.float32)

    def one_wave(wave, carry):
        lines = []
        for part in range(parts):
            even, odd = [], []
            for src in range(grid_count):
                block = rows_ref[src, part, pl.ds(wave, tiles, stride=waves), :]
                piece = [block[i * pairs : (i + 1) * pairs] for i in range(per_pair)]
                even += piece[:half] + [piece[half][:, :64]]
                odd += [piece[half][:, 64:]] + piece[half + 1 :]
            lines += [jnp.concatenate(even, axis=1), jnp.concatenate(odd, axis=1)]
        field = jnp.concatenate(lines, axis=0).astype(jnp.bfloat16)
        basis = legendre_ref[wave]
        coef = lax.dot_general(
            field, basis, (((1,), (1,)), ((), ())), preferred_element_type=jnp.float32
        )
        coef = (coef * response_ref[pl.ds(wave, 1), :]).astype(jnp.bfloat16)
        synth = jnp.dot(coef, basis, preferred_element_type=jnp.float32)
        for part in range(parts):
            even = synth[2 * part * pairs : (2 * part + 1) * pairs]
            odd = synth[(2 * part + 1) * pairs : (2 * part + 2) * pairs]
            for src in range(grid_count):
                base = src * lat_dev
                both = jnp.concatenate(
                    [even[:, base : base + lat_dev], odd[:, base : base + lat_dev]], axis=1
                )
                block = jnp.concatenate(
                    [both[:, i * 128 : (i + 1) * 128] for i in range(per_pair)], axis=0
                )
                back_ref[src, part, pl.ds(wave, tiles, stride=waves), :] = block
        return carry

    lax.fori_loop(0, waves, one_wave, 0, unroll=4)
    for src in range(grid_count):
        for part in range(parts):
            for tile in range(tiles):
                spot = (tile % per_pair) * pairs + tile // per_pair
                out_ref[src, part, :, tile * 128 : (tile + 1) * 128] = back_ref[
                    src, part, spot * waves : (spot + 1) * waves, :
                ].astype(jnp.bfloat16)


def exchange_kernel(
    lat_dev, spectra_ref, legendre_ref, response_ref, result_ref,
    taken_ref, made_ref, basis_ref, rows_ref, back_ref,
    basis_sem, own_sem, send_sem, recv_sem, done_sem, back_send_sem, back_recv_sem,
):
    chunks, grid_count, _, waves, _ = taken_ref.shape
    me = lax.axis_index("grid")
    peers = [lax.rem(me + d, grid_count) for d in range(1, grid_count)]

    def basis_copy(c):
        return pltpu.make_async_copy(legendre_ref.at[c], basis_ref.at[c], basis_sem.at[c])

    def span(c):
        return pl.ds(pl.multiple_of(c * waves, waves), waves)

    def own_copy(c):
        return pltpu.make_async_copy(
            spectra_ref.at[me, :, span(c), :], taken_ref.at[c, me], own_sem.at[c]
        )

    def done_copy(c):
        return pltpu.make_async_copy(
            made_ref.at[c, me], result_ref.at[me, :, span(c), :], done_sem.at[c]
        )

    def out_copy(c, d):
        return pltpu.make_async_remote_copy(
            src_ref=spectra_ref.at[peers[d], :, span(c), :],
            dst_ref=taken_ref.at[c, me],
            send_sem=send_sem.at[c, d],
            recv_sem=recv_sem.at[c, d],
            device_id={"grid": peers[d]},
            device_id_type=pl.DeviceIdType.MESH,
        )

    def back_copy(c, d):
        return pltpu.make_async_remote_copy(
            src_ref=made_ref.at[c, peers[d]],
            dst_ref=result_ref.at[me, :, span(c), :],
            send_sem=back_send_sem.at[c, d],
            recv_sem=back_recv_sem.at[c, d],
            device_id={"grid": peers[d]},
            device_id_type=pl.DeviceIdType.MESH,
        )

    for c in range(chunks):
        basis_copy(c).start()
        own_copy(c).start()
    barrier = pltpu.get_barrier_semaphore()
    for peer in peers:
        pl.semaphore_signal(
            barrier, inc=1, device_id={"grid": peer}, device_id_type=pl.DeviceIdType.MESH
        )
    pl.semaphore_wait(barrier, grid_count - 1)
    for c in range(chunks):
        for d in range(grid_count - 1):
            out_copy(c, d).start()

    def one_chunk(c, carry):
        basis_copy(c).wait()
        own_copy(c).wait()
        for d in range(grid_count - 1):
            out_copy(c, d).wait_recv()
        filter_kernel(
            lat_dev, taken_ref.at[c], basis_ref.at[c], response_ref.at[c], made_ref.at[c], rows_ref, back_ref
        )
        done_copy(c).start()
        for d in range(grid_count - 1):
            back_copy(c, d).start()
        return carry

    lax.fori_loop(0, chunks, one_chunk, 0)
    for c in range(chunks):
        done_copy(c).wait()
        for d in range(grid_count - 1):
            out_copy(c, d).wait_send()
            back_copy(c, d).wait()


def filter_exchanged(spectra, legendre, response, lat_dev):
    grid_count, parts, keep_dev, points = spectra.shape
    degrees, lat_count = legendre.shape[1:]
    waves = 16
    chunks = keep_dev // waves
    stage = pltpu.VMEM((chunks, grid_count, parts, waves, points), jnp.bfloat16)
    turned = pltpu.VMEM((grid_count, parts, points // 128 * waves, 128), jnp.float32)
    one = pltpu.SemaphoreType.DMA((chunks,))
    each = pltpu.SemaphoreType.DMA((chunks, grid_count - 1))
    return pl.pallas_call(
        functools.partial(exchange_kernel, lat_dev),
        out_shape=jax.ShapeDtypeStruct(spectra.shape, jnp.bfloat16),
        in_specs=[
            pl.BlockSpec(memory_space=pl.ANY),
            pl.BlockSpec(memory_space=pl.ANY),
            pl.BlockSpec(memory_space=pltpu.VMEM),
        ],
        out_specs=pl.BlockSpec(memory_space=pl.ANY),
        scratch_shapes=[
            stage, stage, pltpu.VMEM((chunks, waves, degrees, lat_count), jnp.bfloat16), turned, turned,
            one, one, each, each, one, each, each,
        ],
        compiler_params=pltpu.CompilerParams(
            vmem_limit_bytes=56 * 2**20, collective_id=0, has_side_effects=True
        ),
        cost_estimate=pl.CostEstimate(
            flops=2**35, bytes_accessed=2 * keep_dev * degrees * lat_count, transcendentals=0
        ),
    )(
        spectra,
        legendre.reshape(chunks, waves, degrees, lat_count),
        response.reshape(chunks, waves, degrees),
    )


def synth_kernel(where_ref, field_ref, table_ref, weight_ref, give_ref, keep_ref, total_ref):
    member = pl.program_id(1)
    side = where_ref[1]
    pair, lat_dev, wide = total_ref.shape
    values = lax.dot_general(
        field_ref[...], table_ref[...], (((0,), (0,)), ((), ())), preferred_element_type=jnp.float32
    ).reshape(pair, lat_dev, wide)
    term = values * weight_ref[0].astype(jnp.float32)

    @pl.when(member == 0)
    def _():
        total_ref[...] = term

    @pl.when(member > 0)
    def _():
        total_ref[...] += term

    @pl.when(member == pl.num_programs(1) - 1)
    def _():
        give_ref[0] = total_ref[1 - side].astype(jnp.bfloat16)
        keep_ref[0] = total_ref[side]


def synth_pair(filtered, table, perturbation, goal, side):
    mem_dev, levels, lat_dev, lon_count = perturbation.shape
    cols = table.shape[0]
    pairs = levels // 2
    wide = math.gcd(lon_count, 512)
    level = pl.BlockSpec((1, lat_dev, wide), lambda i, k, w: (0, 0, i))
    return pl.pallas_call(
        synth_kernel,
        out_shape=(
            jax.ShapeDtypeStruct((1, lat_dev, lon_count), jnp.bfloat16),
            jax.ShapeDtypeStruct((1, lat_dev, lon_count), jnp.float32),
        ),
        grid_spec=pltpu.PrefetchScalarGridSpec(
            num_scalar_prefetch=1,
            grid=(lon_count // wide, mem_dev),
            in_specs=[
                pl.BlockSpec((cols, 2 * lat_dev), lambda i, k, w: (0, k * pairs + w[0])),
                pl.BlockSpec((cols, wide), lambda i, k, w: (0, i)),
                pl.BlockSpec((1, 2, lat_dev, wide), lambda i, k, w: (k, w[0], 0, i)),
            ],
            out_specs=(level, level),
            scratch_shapes=[pltpu.VMEM((2, lat_dev, wide), jnp.float32)],
        ),
        compiler_params=pltpu.CompilerParams(vmem_limit_bytes=56 * 2**20),
        cost_estimate=pl.CostEstimate(
            flops=4 * mem_dev * lat_dev * cols * lon_count,
            bytes_accessed=4 * mem_dev * lat_dev * lon_count,
            transcendentals=0,
        ),
    )(jnp.stack([goal, side]).astype(jnp.int32), filtered, table, perturbation)


def reduce_pairs(both):
    mem_count = lax.axis_size("mem")
    me = lax.axis_index("mem")
    ring = mem_count // 2
    side, place = me % 2, me // 2
    swap = [(j, j ^ 1) for j in range(mem_count)]
    onward = [(j, (j + 2) % mem_count) for j in range(mem_count)]
    total = None
    for step in range(ring):
        goal = (place + 2 * ring - 1 - step) % ring
        give, here = both(goal, side)
        here = here + lax.ppermute(give, "mem", swap).astype(jnp.float32)
        if total is not None:
            here = here + total.astype(jnp.float32)
        if step < ring - 1:
            total = lax.ppermute(here.astype(jnp.bfloat16), "mem", onward)
    return here


def packed(alpha, perturbation, legendre, response, table):
    mem_dev, levels, lat_dev, lon_count = alpha.shape
    keep_dev = legendre.shape[0]
    grid_count = lax.axis_size("grid")
    points = mem_dev * levels * lat_dev
    spectra = lax.dot_general(
        table, alpha.reshape(points, lon_count), (((1,), (1,)), ((), ())), preferred_element_type=jnp.float32
    ).astype(jnp.bfloat16)
    spectra = spectra.reshape(grid_count, 2, keep_dev, points)
    filtered = filter_exchanged(spectra, legendre, response, lat_dev)
    filtered = filtered.reshape(grid_count * 2 * keep_dev, points)
    return reduce_pairs(lambda goal, side: synth_pair(filtered, table, perturbation, goal, side))


def body(alpha, perturbation, legendre, response):
    mem_dev, levels, lat_dev, lon_count = alpha.shape
    keep_dev = legendre.shape[0]
    grid_count = lax.axis_size("grid")
    members = mem_dev * lax.axis_size("mem")
    cols = 2 * keep_dev
    table = build_table(lon_count, keep_dev, grid_count)
    wave = lax.axis_index("grid") * keep_dev + jnp.arange(keep_dev)
    response = response * jnp.where(wave == 0, 1.0, 2.0).astype(jnp.float32)[:, None]

    scale = jnp.float32(1.0 / (lon_count * math.sqrt(members - 1)))
    if keep_dev % 16 == 0 and lat_dev % 128 == 64 and levels == lax.axis_size("mem") and levels % 2 == 0:
        return packed(alpha, perturbation, legendre, response, table) * scale

    points = mem_dev * levels * lat_dev
    lane = math.gcd(points, 128)
    spectra = jnp.einsum("cx,klyx->ckly", table, alpha, preferred_element_type=jnp.float32)
    spectra = spectra.astype(jnp.bfloat16).reshape(grid_count, cols, points // lane, lane)
    spectra = lax.all_to_all(spectra, "grid", split_axis=0, concat_axis=0, tiled=True)
    split = spectra.reshape(grid_count, 2, keep_dev, mem_dev, levels, lat_dev)
    split = jnp.transpose(split, (1, 2, 3, 4, 0, 5)).reshape(2, keep_dev, mem_dev, levels, -1)
    filtered = legendre_filter(split, legendre, response)
    filtered = filtered.reshape(2, keep_dev, mem_dev, levels, grid_count, lat_dev)
    filtered = jnp.transpose(filtered, (4, 0, 1, 2, 3, 5)).reshape(grid_count, cols, points // lane, lane)
    filtered = lax.all_to_all(filtered, "grid", split_axis=0, concat_axis=0, tiled=True)
    filtered = filtered.reshape(grid_count * cols, mem_dev, levels, lat_dev)
    filtered = jnp.transpose(filtered, (1, 2, 3, 0))

    def partial(level, count):
        field = lax.dynamic_slice_in_dim(filtered, level, count, 1)
        weight = lax.dynamic_slice_in_dim(perturbation, level, count, 1)
        values = jnp.einsum("klyc,cx->klyx", field, table, preferred_element_type=jnp.float32)
        return jnp.sum(values * weight, axis=0)

    total = reduce_levels(partial, levels)
    return total * scale


def solution(mesh):
    placed = (
        P("mem", None, "grid", None),
        P("mem", None, "grid", None),
        P("grid", None, None),
        P("grid", None),
    )
    return jax.shard_map(
        body, mesh=mesh, in_specs=placed, out_specs=P("mem", "grid", None), check_vma=False
    )
```

```python
import functools
import math

import jax
import jax.numpy as jnp
import numpy as np
from jax import lax
from jax.experimental import pallas as pl
from jax.experimental.pallas import tpu as pltpu
from jax.sharding import PartitionSpec as P


def build_table(lon_count, keep_dev, grid_count):
    col = np.arange(2 * keep_dev * grid_count)
    block = col // (2 * keep_dev)
    part = col // keep_dev % 2
    wave = block * keep_dev + col % keep_dev
    phase = wave[:, None] * np.arange(lon_count)[None, :] % lon_count
    angle = phase.astype(np.float32) * np.float32(2.0 * math.pi / lon_count)
    basis = np.where(part[:, None] == 0, np.cos(angle), np.sin(angle))
    return jnp.asarray(basis.astype(jnp.bfloat16))


def legendre_filter(split, legendre, response):
    coef = jnp.einsum("mnt,qmkit->qmkin", legendre, split, preferred_element_type=jnp.float32)
    coef = (coef * response[None, :, None, None, :]).astype(jnp.bfloat16)
    synth = jnp.einsum("mnt,qmkin->qmkit", legendre, coef, preferred_element_type=jnp.float32)
    return synth.astype(jnp.bfloat16)


def reduce_levels(partial, levels):
    mem_count = lax.axis_size("mem")
    me = lax.axis_index("mem")
    owned = levels // mem_count
    if mem_count % 2:
        every = jnp.concatenate([partial(i * owned, owned) for i in range(mem_count)])
        return lax.psum_scatter(every, "mem", scatter_dimension=0, tiled=True)
    ring = mem_count // 2
    side, place = me % 2, me // 2
    swap = [(j, j ^ 1) for j in range(mem_count)]
    onward = [(j, (j + 2) % mem_count) for j in range(mem_count)]
    total = None
    for step in range(ring):
        goal = (place + 2 * ring - 1 - step) % ring
        give = partial((2 * goal + 1 - side) * owned, owned).astype(jnp.bfloat16)
        got = lax.ppermute(give, "mem", swap)
        here = partial((2 * goal + side) * owned, owned)
        here = here + got.astype(jnp.float32)
        if total is not None:
            here = here + total.astype(jnp.float32)
        if step < ring - 1:
            total = lax.ppermute(here.astype(jnp.bfloat16), "mem", onward)
    return here


def filter_kernel(lat_dev, x_ref, legendre_ref, response_ref, out_ref, rows_ref, back_ref):
    grid_count, parts, waves, points = x_ref.shape
    tiles = points // 128
    per_pair = 2 * lat_dev // 128
    pairs = tiles // per_pair
    half = per_pair // 2
    for src in range(grid_count):
        for part in range(parts):
            for tile in range(tiles):
                spot = (tile % per_pair) * pairs + tile // per_pair
                rows_ref[src, part, spot * waves : (spot + 1) * waves, :] = x_ref[
                    src, part, :, tile * 128 : (tile + 1) * 128
                ].astype(jnp.float32)

    def one_wave(wave, carry):
        lines = []
        for part in range(parts):
            even, odd = [], []
            for src in range(grid_count):
                block = rows_ref[src, part, pl.ds(wave, tiles, stride=waves), :]
                piece = [block[i * pairs : (i + 1) * pairs] for i in range(per_pair)]
                even += piece[:half] + [piece[half][:, :64]]
                odd += [piece[half][:, 64:]] + piece[half + 1 :]
            lines += [jnp.concatenate(even, axis=1), jnp.concatenate(odd, axis=1)]
        field = jnp.concatenate(lines, axis=0).astype(jnp.bfloat16)
        basis = legendre_ref[wave]
        coef = lax.dot_general(
            field, basis, (((1,), (1,)), ((), ())), preferred_element_type=jnp.float32
        )
        coef = (coef * response_ref[pl.ds(wave, 1), :]).astype(jnp.bfloat16)
        synth = jnp.dot(coef, basis, preferred_element_type=jnp.float32)
        for part in range(parts):
            even = synth[2 * part * pairs : (2 * part + 1) * pairs]
            odd = synth[(2 * part + 1) * pairs : (2 * part + 2) * pairs]
            for src in range(grid_count):
                base = src * lat_dev
                both = jnp.concatenate(
                    [even[:, base : base + lat_dev], odd[:, base : base + lat_dev]], axis=1
                )
                block = jnp.concatenate(
                    [both[:, i * 128 : (i + 1) * 128] for i in range(per_pair)], axis=0
                )
                back_ref[src, part, pl.ds(wave, tiles, stride=waves), :] = block
        return carry

    lax.fori_loop(0, waves, one_wave, 0, unroll=4)
    for src in range(grid_count):
        for part in range(parts):
            for tile in range(tiles):
                spot = (tile % per_pair) * pairs + tile // per_pair
                out_ref[src, part, :, tile * 128 : (tile + 1) * 128] = back_ref[
                    src, part, spot * waves : (spot + 1) * waves, :
                ].astype(jnp.bfloat16)


def exchange_kernel(
    lat_dev, spectra_ref, legendre_ref, response_ref, result_ref,
    taken_ref, made_ref, basis_ref, rows_ref, back_ref,
    basis_sem, own_sem, send_sem, recv_sem, done_sem, back_send_sem, back_recv_sem,
):
    chunks, grid_count, _, waves, _ = taken_ref.shape
    me = lax.axis_index("grid")
    peers = [lax.rem(me + d, grid_count) for d in range(1, grid_count)]

    def basis_copy(c):
        return pltpu.make_async_copy(legendre_ref.at[c], basis_ref.at[c], basis_sem.at[c])

    def span(c):
        return pl.ds(pl.multiple_of(c * waves, waves), waves)

    def own_copy(c):
        return pltpu.make_async_copy(
            spectra_ref.at[me, :, span(c), :], taken_ref.at[c, me], own_sem.at[c]
        )

    def done_copy(c):
        return pltpu.make_async_copy(
            made_ref.at[c, me], result_ref.at[me, :, span(c), :], done_sem.at[c]
        )

    def out_copy(c, d):
        return pltpu.make_async_remote_copy(
            src_ref=spectra_ref.at[peers[d], :, span(c), :],
            dst_ref=taken_ref.at[c, me],
            send_sem=send_sem.at[c, d],
            recv_sem=recv_sem.at[c, d],
            device_id={"grid": peers[d]},
            device_id_type=pl.DeviceIdType.MESH,
        )

    def back_copy(c, d):
        return pltpu.make_async_remote_copy(
            src_ref=made_ref.at[c, peers[d]],
            dst_ref=result_ref.at[me, :, span(c), :],
            send_sem=back_send_sem.at[c, d],
            recv_sem=back_recv_sem.at[c, d],
            device_id={"grid": peers[d]},
            device_id_type=pl.DeviceIdType.MESH,
        )

    for c in range(chunks):
        basis_copy(c).start()
        own_copy(c).start()
    barrier = pltpu.get_barrier_semaphore()
    for peer in peers:
        pl.semaphore_signal(
            barrier, inc=1, device_id={"grid": peer}, device_id_type=pl.DeviceIdType.MESH
        )
    pl.semaphore_wait(barrier, grid_count - 1)
    for c in range(chunks):
        for d in range(grid_count - 1):
            out_copy(c, d).start()

    def one_chunk(c, carry):
        basis_copy(c).wait()
        own_copy(c).wait()
        for d in range(grid_count - 1):
            out_copy(c, d).wait_recv()
        filter_kernel(
            lat_dev, taken_ref.at[c], basis_ref.at[c], response_ref.at[c], made_ref.at[c], rows_ref, back_ref
        )
        done_copy(c).start()
        for d in range(grid_count - 1):
            back_copy(c, d).start()
        return carry

    lax.fori_loop(0, chunks, one_chunk, 0)
    for c in range(chunks):
        done_copy(c).wait()
        for d in range(grid_count - 1):
            out_copy(c, d).wait_send()
            back_copy(c, d).wait()


def filter_exchanged(spectra, legendre, response, lat_dev):
    grid_count, parts, keep_dev, points = spectra.shape
    degrees, lat_count = legendre.shape[1:]
    waves = 16
    chunks = keep_dev // waves
    stage = pltpu.VMEM((chunks, grid_count, parts, waves, points), jnp.bfloat16)
    turned = pltpu.VMEM((grid_count, parts, points // 128 * waves, 128), jnp.float32)
    one = pltpu.SemaphoreType.DMA((chunks,))
    each = pltpu.SemaphoreType.DMA((chunks, grid_count - 1))
    return pl.pallas_call(
        functools.partial(exchange_kernel, lat_dev),
        out_shape=jax.ShapeDtypeStruct(spectra.shape, jnp.bfloat16),
        in_specs=[
            pl.BlockSpec(memory_space=pl.ANY),
            pl.BlockSpec(memory_space=pl.ANY),
            pl.BlockSpec(memory_space=pltpu.VMEM),
        ],
        out_specs=pl.BlockSpec(memory_space=pl.ANY),
        scratch_shapes=[
            stage, stage, pltpu.VMEM((chunks, waves, degrees, lat_count), jnp.bfloat16), turned, turned,
            one, one, each, each, one, each, each,
        ],
        compiler_params=pltpu.CompilerParams(
            vmem_limit_bytes=56 * 2**20, collective_id=0, has_side_effects=True
        ),
        cost_estimate=pl.CostEstimate(
            flops=2**35, bytes_accessed=2 * keep_dev * degrees * lat_count, transcendentals=0
        ),
    )(
        spectra,
        legendre.reshape(chunks, waves, degrees, lat_count),
        response.reshape(chunks, waves, degrees),
    )


def synth_kernel(where_ref, field_ref, table_ref, weight_ref, give_ref, keep_ref, total_ref):
    member = pl.program_id(1)
    side = where_ref[1]
    pair, lat_dev, wide = total_ref.shape
    values = lax.dot_general(
        field_ref[...], table_ref[...], (((0,), (0,)), ((), ())), preferred_element_type=jnp.float32
    ).reshape(pair, lat_dev, wide)
    term = values * weight_ref[0].astype(jnp.float32)

    @pl.when(member == 0)
    def _():
        total_ref[...] = term

    @pl.when(member > 0)
    def _():
        total_ref[...] += term

    @pl.when(member == pl.num_programs(1) - 1)
    def _():
        give_ref[0] = total_ref[1 - side].astype(jnp.bfloat16)
        keep_ref[0] = total_ref[side]


def synth_pair(filtered, table, perturbation, goal, side, strip, strips):
    mem_dev, levels, lat_dev, lon_count = perturbation.shape
    cols = table.shape[0]
    pairs = levels // 2
    strip_lon = lon_count // strips
    wide = strip_lon
    first = strip * (strip_lon // wide)
    level = pl.BlockSpec((1, lat_dev, wide), lambda i, k, w: (0, 0, i))
    return pl.pallas_call(
        synth_kernel,
        out_shape=(
            jax.ShapeDtypeStruct((1, lat_dev, strip_lon), jnp.bfloat16),
            jax.ShapeDtypeStruct((1, lat_dev, strip_lon), jnp.float32),
        ),
        grid_spec=pltpu.PrefetchScalarGridSpec(
            num_scalar_prefetch=1,
            grid=(strip_lon // wide, mem_dev),
            in_specs=[
                pl.BlockSpec((cols, 2 * lat_dev), lambda i, k, w: (0, k * pairs + w[0])),
                pl.BlockSpec((cols, wide), lambda i, k, w: (0, i + first)),
                pl.BlockSpec((1, 2, lat_dev, wide), lambda i, k, w: (k, w[0], 0, i + first)),
            ],
            out_specs=(level, level),
            scratch_shapes=[pltpu.VMEM((2, lat_dev, wide), jnp.float32)],
        ),
        compiler_params=pltpu.CompilerParams(vmem_limit_bytes=56 * 2**20),
        cost_estimate=pl.CostEstimate(
            flops=4 * mem_dev * lat_dev * cols * strip_lon,
            bytes_accessed=4 * mem_dev * lat_dev * strip_lon,
            transcendentals=0,
        ),
    )(jnp.stack([goal, side]).astype(jnp.int32), filtered, table, perturbation)


def reduce_pairs(both, strips):
    mem_count = lax.axis_size("mem")
    me = lax.axis_index("mem")
    ring = mem_count // 2
    side, place = me % 2, me // 2
    swap = [(j, j ^ 1) for j in range(mem_count)]
    onward = [(j, (j + 2) % mem_count) for j in range(mem_count)]
    totals = [None] * strips
    for step in range(ring):
        goal = (place + 2 * ring - 1 - step) % ring
        for strip in range(strips):
            give, here = both(goal, side, strip)
            here = here + lax.ppermute(give, "mem", swap).astype(jnp.float32)
            if step > 0:
                here = here + totals[strip].astype(jnp.float32)
            if step < ring - 1:
                here = lax.ppermute(here.astype(jnp.bfloat16), "mem", onward)
            totals[strip] = here
    return jnp.concatenate(totals, axis=2)


def packed(alpha, perturbation, legendre, response, table):
    mem_dev, levels, lat_dev, lon_count = alpha.shape
    keep_dev = legendre.shape[0]
    grid_count = lax.axis_size("grid")
    points = mem_dev * levels * lat_dev
    spectra = lax.dot_general(
        table, alpha.reshape(points, lon_count), (((1,), (1,)), ((), ())), preferred_element_type=jnp.float32
    ).astype(jnp.bfloat16)
    spectra = spectra.reshape(grid_count, 2, keep_dev, points)
    filtered = filter_exchanged(spectra, legendre, response, lat_dev)
    filtered = filtered.reshape(grid_count * 2 * keep_dev, points)
    strips = 2 if lon_count % 256 == 0 else 1

    def both(goal, side, strip):
        return synth_pair(filtered, table, perturbation, goal, side, strip, strips)

    return reduce_pairs(both, strips)


def body(alpha, perturbation, legendre, response):
    mem_dev, levels, lat_dev, lon_count = alpha.shape
    keep_dev = legendre.shape[0]
    grid_count = lax.axis_size("grid")
    members = mem_dev * lax.axis_size("mem")
    cols = 2 * keep_dev
    table = build_table(lon_count, keep_dev, grid_count)
    wave = lax.axis_index("grid") * keep_dev + jnp.arange(keep_dev)
    response = response * jnp.where(wave == 0, 1.0, 2.0).astype(jnp.float32)[:, None]

    scale = jnp.float32(1.0 / (lon_count * math.sqrt(members - 1)))
    if keep_dev % 16 == 0 and lat_dev % 128 == 64 and levels == lax.axis_size("mem") and levels % 2 == 0:
        return packed(alpha, perturbation, legendre, response, table) * scale

    points = mem_dev * levels * lat_dev
    lane = math.gcd(points, 128)
    spectra = jnp.einsum("cx,klyx->ckly", table, alpha, preferred_element_type=jnp.float32)
    spectra = spectra.astype(jnp.bfloat16).reshape(grid_count, cols, points // lane, lane)
    spectra = lax.all_to_all(spectra, "grid", split_axis=0, concat_axis=0, tiled=True)
    split = spectra.reshape(grid_count, 2, keep_dev, mem_dev, levels, lat_dev)
    split = jnp.transpose(split, (1, 2, 3, 4, 0, 5)).reshape(2, keep_dev, mem_dev, levels, -1)
    filtered = legendre_filter(split, legendre, response)
    filtered = filtered.reshape(2, keep_dev, mem_dev, levels, grid_count, lat_dev)
    filtered = jnp.transpose(filtered, (4, 0, 1, 2, 3, 5)).reshape(grid_count, cols, points // lane, lane)
    filtered = lax.all_to_all(filtered, "grid", split_axis=0, concat_axis=0, tiled=True)
    filtered = filtered.reshape(grid_count * cols, mem_dev, levels, lat_dev)
    filtered = jnp.transpose(filtered, (1, 2, 3, 0))

    def partial(level, count):
        field = lax.dynamic_slice_in_dim(filtered, level, count, 1)
        weight = lax.dynamic_slice_in_dim(perturbation, level, count, 1)
        values = jnp.einsum("klyc,cx->klyx", field, table, preferred_element_type=jnp.float32)
        return jnp.sum(values * weight, axis=0)

    total = reduce_levels(partial, levels)
    return total * scale


def solution(mesh):
    placed = (
        P("mem", None, "grid", None),
        P("mem", None, "grid", None),
        P("grid", None, None),
        P("grid", None),
    )
    return jax.shard_map(
        body, mesh=mesh, in_specs=placed, out_specs=P("mem", "grid", None), check_vma=False
    )
```
